32 devices in a mesh: seq: 8 (over z, x), head: 4 (over y, core).
Axes of the slice: x: 2, y: 2, z: 4, core: 2. Of those that a mesh axis runs over, the one named last changes fastest.
Arguments:
- queries: bfloat16 [4096, 6144], P('seq', 'head'), may hold values from -10 to 10
- keys: bfloat16 [4096, 6144], P('seq', 'head'), may hold values from -10 to 10
- values: bfloat16 [4096, 6144], P('seq', 'head'), may hold values from -6 to 6
- frame_of_block: int32 [16], P('seq'), may hold values from 0 to 7, never falling along the last dimension, each value on 1 to 4 neighbouring positions
- pair_mask: int32 [16, 16], P('seq'), may hold values 0 or 1
- w_out: bfloat16 [6144, 6144], P('head', 'seq'), may hold values from -0.4375 to 0.4375
Outputs:
- projected: bfloat16 [4096, 6144], P('seq', 'head')
The draws below stay inside these ranges and needn't reach their ends.
Inputs may be any that keep to these rules, and one draw needn't show every extreme that they name: `frame_of_block`: frame ids never fall along the blocks, every frame spans 1 to 4 consecutive blocks.
All inputs are finite; a program needn't handle non-finite values. No bound on the sum of `pair_mask` on one device may be relied on, other than what follows from the above.
Results may differ from the reference program's by a relative error of at most 0.015.
Values may be sent and summed in bfloat16 or wider, within the bound.
No kernel may reach another device: no remote copies, remote signals or barrier semaphores. Data moves between devices by JAX's collectives and lax.ppermute only.
A program may use at most 192 MiB of HBM per device.

```python
import math
import jax
import jax.numpy as jnp
import numpy as np
from jax import lax

D = 6144
H = 48
HD = 128
BLK = 256
TOK_DEV = 512
TOKENS = 4096
NBLK = 16
FRAMES = 8


def joint_draw(key):
    width = H * HD
    q_draw = jnp.clip(1.5 * jax.random.normal(jax.random.fold_in(key, 101), (TOKENS, width), jnp.float32), -6.0, 6.0)
    k_draw = jnp.clip(1.5 * jax.random.normal(jax.random.fold_in(key, 202), (TOKENS, width), jnp.float32), -6.0, 6.0)
    return (q_draw, k_draw)


def draw_queries(key, part):
    return joint_draw(key)[0].astype(jnp.bfloat16)


def draw_keys(key, part):
    return joint_draw(key)[1].astype(jnp.bfloat16)


def touch_ends(result, stream_key, least, largest):
    spot = [jax.random.randint(jax.random.fold_in(stream_key, axis), (), 0, length) for axis, length in enumerate(result.shape)]
    main_axis = result.shape.index(max(result.shape))
    beside = spot[:main_axis] + [(spot[main_axis] + 1) % result.shape[main_axis]] + spot[main_axis + 1:]
    return result.at[tuple(spot)].set(least).at[tuple(beside)].set(largest)


def shard_levels(own_key, extent, shards, low, largest):
    factor_of, own = 1.0, jax.random.fold_in(own_key, 6)
    for dim, parts in shards:
        steps = jnp.exp(jax.random.uniform(jax.random.fold_in(own, dim), (parts,), jnp.float32, low / len(shards), largest / len(shards)))
        factor_of = factor_of * jnp.repeat(steps, extent[dim] // parts).reshape([-1 if axis == dim else 1 for axis in range(len(extent))])
    return factor_of


def length_profile(count, total, most, slope):
    weights = [(1 << 20) // math.isqrt(standing ** slope) + 1 for standing in range(2, count + 1)]
    spare, given = total - most - (count - 1), [1] * (count - 1)
    while spare > 0:
        movable = [i for i in range(count - 1) if given[i] < most]
        mass, left = sum([weights[i] for i in movable]), spare
        for i in movable:
            more = min(most - given[i], max(1, left * weights[i] // mass), spare)
            given[i] = given[i] + more
            spare = spare - more
    return np.array([most] + given)


def uneven_parts(key, amount, total, reach, skew):
    if amount == 2:
        one = jax.random.randint(key, (), max(1, total - reach), min(reach, total - 1) + 1)
        return jnp.stack([one, total - one])
    tallies = jnp.asarray(length_profile(amount, total, reach, skew), jnp.int32)
    twos = (amount - 1) // 2
    giver, sink = tallies[1:1 + 2 * twos:2], tallies[2:2 + 2 * twos:2]
    slack = jnp.minimum(giver - 1, reach - sink)
    shifted = jax.random.randint(jax.random.fold_in(key, 1), (twos,), 0, 1 << 20) % (slack + 1)
    tallies = tallies.at[1:1 + 2 * twos:2].set(giver - shifted).at[2:2 + 2 * twos:2].set(sink + shifted)
    return tallies[jax.random.permutation(jax.random.fold_in(key, 2), amount)]


def noise(stream_key, dims, scale, most, pieces=(), kind=jnp.bfloat16):
    values = scale * jax.random.normal(stream_key, dims, jnp.float32)
    if pieces:
        values = values * shard_levels(stream_key, dims, pieces, -0.22, 0.18)
    return jnp.clip(values, -most, most).astype(kind)


def setup_inputs(seed: int = 0) -> dict:
    key_of = jax.random.split(jax.random.key(seed), 7)
    return {
        "queries": draw_queries(jax.random.fold_in(key_of[6], 71), 0),
        "keys": draw_keys(jax.random.fold_in(key_of[6], 71), 0),
        "values": noise(key_of[2], (TOKENS, D), 1.0, 6.0, ((0, 8), (1, 4))),
        "frame_of_block": jnp.searchsorted(jnp.cumsum(uneven_parts(key_of[3], FRAMES, NBLK, 4, 1)), jnp.arange(NBLK), side="right").astype(jnp.int32),
        "pair_mask": touch_ends((jax.random.randint(key_of[4], (NBLK, NBLK), 0, 4) < 3).astype(jnp.int32), jax.random.fold_in(key_of[4], 1), 0, 1),
        "w_out": noise(key_of[5], (D, D), (D // 32) ** -0.5, 0.4375, ((0, 4), (1, 8))),
    }


def reference(queries, keys, values, frame_of_block, pair_mask, w_out):
    width = H * HD
    scale = 1.0 / math.sqrt(HD)
    tok_frame = jnp.repeat(frame_of_block, BLK)
    key_block = (jnp.arange(TOKENS, dtype=jnp.int32) // BLK).astype(jnp.int32)
    count_blocks = TOKENS // TOK_DEV

    def one_block(index):
        first = (index * TOK_DEV).astype(jnp.int32)
        rows = lax.dynamic_slice_in_dim(queries, first, TOK_DEV, 0)
        q_frame = lax.dynamic_slice_in_dim(tok_frame, first, TOK_DEV, 0)
        q_block = ((first + jnp.arange(TOK_DEV, dtype=jnp.int32)) // BLK).astype(jnp.int32)
        link = pair_mask[q_block][:, key_block]
        allowed = (tok_frame[None, :] <= q_frame[:, None]) & ((link == 1) | (tok_frame[None, :] == q_frame[:, None]))

        def one_head(head_index):
            col = (head_index * HD).astype(jnp.int32)
            q_head = lax.dynamic_slice_in_dim(rows, col, HD, 1)
            k_head = lax.dynamic_slice_in_dim(keys, col, HD, 1)
            v_head = lax.dynamic_slice_in_dim(values, col, HD, 1)
            score = jnp.dot(q_head, k_head.T, preferred_element_type=jnp.float32) * scale
            score = jnp.where(allowed, score, -1e+30)
            peak = lax.optimization_barrier(jnp.max(score, axis=1))
            weight = jnp.where(allowed, jnp.exp(score - peak[:, None]), 0.0)
            total = lax.optimization_barrier(jnp.sum(weight, axis=1))
            mixed = jnp.dot(weight.astype(jnp.bfloat16), v_head, preferred_element_type=jnp.float32)
            return mixed / total[:, None]
        heads = lax.map(one_head, jnp.arange(H, dtype=jnp.int32))
        return jnp.transpose(heads, (1, 0, 2)).reshape(TOK_DEV, width).astype(jnp.bfloat16)
    attn = lax.map(one_block, jnp.arange(count_blocks, dtype=jnp.int32)).reshape(TOKENS, width)
    return jnp.dot(attn, w_out, preferred_element_type=jnp.float32).astype(jnp.bfloat16)
```

```python
import functools
import math

import jax
import jax.numpy as jnp
from jax import lax
from jax.experimental import pallas as pl
from jax.experimental.pallas import tpu as pltpu
from jax.sharding import PartitionSpec as P

HD = 128
BLK = 256
SPAN = 4
META = 16
BOTH = ("seq", "head")


def attention_kernel(devices, group, tok, count, order, *refs):
    pieces, out, q_all, k_all, v_all, peak, total, accum, sems = (refs[:devices], *refs[devices:])
    copies = []
    for d in range(devices):
        parts = ((k_all, 0), (v_all, tok), (q_all, 2 * tok + META))
        for part, (held, first) in enumerate(parts[: 3 if d < group else 2]):
            copies.append(
                pltpu.make_async_copy(
                    pieces[d].at[pl.ds(first, tok)], held.at[pl.ds(d * tok, tok)], sems.at[3 * d + part]
                )
            )
    for copy in copies:
        copy.start()
    for copy in copies:
        copy.wait()
    factor = math.log2(math.e) / math.sqrt(HD)
    key_blocks = devices * tok // BLK

    @pl.loop(0, group * tok // BLK)
    def _(index):
        rows = pl.ds(pl.multiple_of(index * BLK, BLK), BLK)
        q = q_all[rows, :]
        seen = count[index]
        peak[...] = jnp.full_like(peak, -jnp.inf)
        total[...] = jnp.zeros_like(total)
        accum[...] = jnp.zeros_like(accum)

        def update(step, number):
            firsts = [
                pl.multiple_of(order[index * key_blocks + step + u] * BLK, BLK) for u in range(number)
            ]
            scores = [
                lax.dot_general(
                    q, k_all[pl.ds(first, BLK), :], (((1,), (1,)), ((), ())), preferred_element_type=jnp.float32
                )
                for first in firsts
            ]
            top = functools.reduce(jnp.maximum, [s[:, i : i + HD] for s in scores for i in (0, HD)])
            old = peak[...]
            new = jnp.maximum(old, jnp.broadcast_to(jnp.max(top, axis=1, keepdims=True), old.shape))
            peak[...] = new
            fade = jnp.exp2((old - new) * factor)
            sums, mixed = None, None
            for first, score in zip(firsts, scores):
                left = jnp.exp2((score[:, :HD] - new) * factor)
                right = jnp.exp2((score[:, HD:] - new) * factor)
                weight = jnp.concatenate([left.astype(jnp.bfloat16), right.astype(jnp.bfloat16)], axis=1)
                term = jnp.dot(weight, v_all[pl.ds(first, BLK), :], preferred_element_type=jnp.float32)
                sums = left + right if sums is None else sums + (left + right)
                mixed = term if mixed is None else mixed + term
            total[...] = total[...] * fade + sums
            accum[...] = accum[...] * fade + mixed

        @pl.loop(0, seen // 4)
        def _(step):
            update(step * 4, 4)

        @pl.when((seen & 2) != 0)
        def _():
            update((seen // 4) * 4, 2)

        @pl.when((seen & 1) != 0)
        def _():
            update(seen - 1, 1)

        out[rows, :] = (accum[...] / jnp.sum(total[...], axis=1, keepdims=True)).astype(out.dtype)


def attend_head(count, order, pieces, group, tok):
    devices = len(pieces)
    rows, keys = group * tok, devices * tok
    return pl.pallas_call(
        functools.partial(attention_kernel, devices, group, tok),
        out_shape=jax.ShapeDtypeStruct((rows, HD), jnp.bfloat16),
        in_specs=[pl.BlockSpec(memory_space=pltpu.SMEM)] * 2 + [pl.BlockSpec(memory_space=pl.ANY)] * devices,
        out_specs=pl.BlockSpec(memory_space=pltpu.VMEM),
        scratch_shapes=[
            pltpu.VMEM((rows, HD), jnp.bfloat16),
            pltpu.VMEM((keys, HD), jnp.bfloat16),
            pltpu.VMEM((keys, HD), jnp.bfloat16),
            pltpu.VMEM((BLK, HD), jnp.float32),
            pltpu.VMEM((BLK, HD), jnp.float32),
            pltpu.VMEM((BLK, HD), jnp.float32),
            pltpu.SemaphoreType.DMA((3 * devices,)),
        ],
        compiler_params=pltpu.CompilerParams(vmem_limit_bytes=24 << 20),
        cost_estimate=pl.CostEstimate(
            flops=4 * rows * keys * HD, bytes_accessed=2 * HD * (2 * rows + 2 * keys), transcendentals=rows * keys
        ),
        name="attend_head",
    )(count, order, *pieces)


def pack_kernel(group, share, tok, own, keys, values, queries, meta, *refs):
    number = group * share
    whole, short = refs[:number], refs[number : 2 * number]
    held, in_sems, out_sems = refs[2 * number :]
    rows = ((keys, 0, tok), (values, tok, tok), (meta, 2 * tok, META), (queries, 2 * tok + META, tok))
    takes, puts = [], []
    for c in range(group):
        for t in range(share):
            i = c * share + t
            first = pl.multiple_of(((own[0] ^ c) * share + t) * HD, HD)
            takes.append(
                [
                    pltpu.make_async_copy(
                        source if source is meta else source.at[:, pl.ds(first, HD)],
                        held.at[i, pl.ds(start, size)],
                        in_sems.at[4 * i + part],
                    )
                    for part, (source, start, size) in enumerate(rows)
                ]
            )
            puts.append(
                [
                    pltpu.make_async_copy(held.at[i], whole[i], out_sems.at[2 * i]),
                    pltpu.make_async_copy(held.at[i, pl.ds(0, 2 * tok + META)], short[i], out_sems.at[2 * i + 1]),
                ]
            )
    for i in [c * share + t for t in range(share) for c in range(group)]:
        for copy in takes[i]:
            copy.start()
    for i in [c * share + t for t in range(share) for c in range(group)]:
        for copy in takes[i]:
            copy.wait()
        for copy in puts[i]:
            copy.start()
    for pair in puts:
        for copy in pair:
            copy.wait()


def pack(own, keys, values, queries, meta, group, share):
    tok = keys.shape[0]
    number = group * share
    sizes = [3 * tok + META] * number + [2 * tok + META] * number
    packed = pl.pallas_call(
        functools.partial(pack_kernel, group, share, tok),
        out_shape=[jax.ShapeDtypeStruct((size, HD), jnp.bfloat16) for size in sizes],
        in_specs=[pl.BlockSpec(memory_space=pltpu.SMEM)] + [pl.BlockSpec(memory_space=pl.ANY)] * 4,
        out_specs=[pl.BlockSpec(memory_space=pl.ANY)] * (2 * number),
        scratch_shapes=[
            pltpu.VMEM((number, 3 * tok + META, HD), jnp.bfloat16),
            pltpu.SemaphoreType.DMA((4 * number,)),
            pltpu.SemaphoreType.DMA((2 * number,)),
        ],
        compiler_params=pltpu.CompilerParams(vmem_limit_bytes=16 << 20),
        name="pack",
    )(own[None], keys, values, queries, meta)
    split = lambda flat: [flat[c * share : (c + 1) * share] for c in range(group)]
    return split(packed[:number]), split(packed[number:])


def block_lists(k_frame, rows, held, valid):
    number = held.shape[0]
    q_frame = k_frame[: rows.shape[0]]
    pick = (held[:, None] == jnp.arange(rows.shape[1], dtype=jnp.int32)[None, :]).astype(jnp.int32)
    link = jnp.sum(rows[:, None, :] * pick[None, :, :], axis=2)
    same = k_frame[None, :] == q_frame[:, None]
    allowed = (k_frame[None, :] <= q_frame[:, None]) & ((link == 1) | same) & valid[None, :]
    seen = allowed.astype(jnp.int32)
    spot = jnp.arange(number, dtype=jnp.int32)
    before = (spot[:, None] < spot[None, :]).astype(jnp.int32)
    rank = jnp.sum(seen[:, :, None] * before[None, :, :], axis=1)
    chosen = seen[:, :, None] * (rank[:, :, None] == spot[None, None, :]).astype(jnp.int32)
    order = jnp.sum(chosen * spot[None, :, None], axis=1)
    return jnp.sum(seen, axis=1), order.reshape(-1)


def halves_body(queries, keys, values, frame_of_block, pair_mask, w_out, devices):
    group = devices // 2
    tok, width = queries.shape
    heads = width // HD
    share = heads // group
    per_dev = frame_of_block.shape[0]
    near = -(-(SPAN - 1) // per_dev)
    seq, head = lax.axis_index("seq"), lax.axis_index("head")
    own = lax.rem(seq, group)
    half, side, core = seq // group, head // 2, lax.rem(head, 2)

    meta = jnp.concatenate([frame_of_block[:, None], pair_mask], axis=1).astype(jnp.bfloat16)
    blocks = pair_mask.shape[1]
    meta = jnp.pad(meta, ((0, META - per_dev), (0, HD - 1 - blocks)))
    whole, short = pack(own, keys, values, queries, meta, group, share)

    arrived = []
    for t in range(share):
        row = [whole[0][t]]
        for d in range(1, devices):
            if d < group:
                row.append(lax.ppermute(whole[d][t], "seq", [(s, s ^ d) for s in range(devices)]))
            else:
                row.append(lax.ppermute(short[d % group][t], "seq", [(s, s ^ d) for s in range(group + near)]))
        arrived.append(row)

    told = [piece[2 * tok : 2 * tok + per_dev, : 1 + blocks].astype(jnp.int32) for piece in arrived[0]]
    told = jnp.concatenate(told, axis=0)
    source = seq ^ jnp.arange(devices, dtype=jnp.int32)
    held = (source[:, None] * per_dev + jnp.arange(per_dev, dtype=jnp.int32)).reshape(-1)
    valid = (half == 1) | (held < (group + near) * per_dev)
    count, order = block_lists(told[:, 0], told[: group * per_dev, 1:], held, valid)

    columns = w_out.shape[1]
    w_here = jnp.concatenate(
        [lax.dynamic_slice_in_dim(w_out, (own ^ e) * share * HD, share * HD, 0) for e in range(group)], axis=0
    )
    parts = 2
    step = columns // parts
    w_far = [
        lax.ppermute(w_here[:, p * step : (p + 1) * step], "seq", [(s, s ^ group) for s in range(devices)])
        for p in range(parts)
    ]

    gathered = [[None] * share for _ in range(group)]
    for t in range(share):
        mixed = attend_head(count, order, arrived[t], group, tok)
        gathered[0][t] = mixed
        for e in range(1, group):
            gathered[e][t] = lax.ppermute(mixed, "seq", [(s, s ^ e) for s in range(devices)])
    attn = jnp.concatenate(
        [
            jnp.concatenate(
                [gathered[e][t][(d ^ e) * tok : ((d ^ e) + 1) * tok] for e in range(group) for t in range(share)],
                axis=1,
            )
            for d in range(group)
        ],
        axis=0,
    )

    pairs = [(s, h) for s in range(devices) for h in range(4)]

    def place(s, h):
        return s * 4 + h

    def finish(weights, near_side):
        sides = [(s, h) for s, h in pairs if (h // 2 == s // group) == near_side]
        terms = jnp.dot(attn, weights, preferred_element_type=jnp.float32)
        kept = lax.dynamic_slice_in_dim(terms, core * 2 * tok, 2 * tok, 0)
        given = lax.dynamic_slice_in_dim(terms, (1 - core) * 2 * tok, 2 * tok, 0).astype(jnp.bfloat16)
        kept = kept + lax.ppermute(given, "head", [(h, h ^ 1) for h in range(4)]).astype(jnp.float32)
        other = lax.ppermute(
            kept.astype(jnp.bfloat16), BOTH, [(place(s, h ^ 2), place(s, h)) for s, h in sides]
        )
        summed = (kept + other.astype(jnp.float32)).astype(jnp.bfloat16)
        ends = []
        for flip in range(2):
            moves = [
                (place(s, h), place(s ^ ((h % 2) * 2 + flip), (h // 2) * 2 + (s % group) // 2)) for s, h in sides
            ]
            ends.append(lax.ppermute(summed[flip * tok : (flip + 1) * tok], BOTH, moves))
        return ends

    near_ends = finish(w_here, True)
    far_parts = [finish(w, False) for w in w_far]
    far_ends = [jnp.concatenate([part[flip] for part in far_parts], axis=1) for flip in range(2)]
    same, across = [jnp.where(half == side, n, f) for n, f in zip(near_ends, far_ends)]
    odd = lax.rem(seq, 2) == 1
    return jnp.concatenate([jnp.where(odd, across, same), jnp.where(odd, same, across)], axis=1)


def gather_body(queries, keys, values, frame_of_block, pair_mask, w_out, devices):
    tok, width = queries.shape
    heads = width // HD
    per_dev = frame_of_block.shape[0]
    seq = lax.axis_index("seq")
    meta = lax.all_gather(jnp.concatenate([frame_of_block[:, None], pair_mask], axis=1), "seq", axis=0, tiled=True)
    source = seq ^ jnp.arange(devices, dtype=jnp.int32)
    held = (source[:, None] * per_dev + jnp.arange(per_dev, dtype=jnp.int32)).reshape(-1)
    pick = (held[:, None] == jnp.arange(devices * per_dev, dtype=jnp.int32)[None, :]).astype(jnp.int32)
    k_frame = jnp.sum(pick * meta[None, :, 0], axis=1)
    count, order = block_lists(k_frame, pair_mask, held, held >= 0)
    split = [x.reshape(tok, heads, HD).transpose(1, 0, 2) for x in (keys, values, queries)]
    stacked = jnp.concatenate(split[:2] + [jnp.zeros((heads, META, HD), jnp.bfloat16), split[2]], axis=1)
    pairs = [[(s, s ^ d) for s in range(devices)] for d in range(devices)]
    mixed = []
    for t in range(heads):
        row = [stacked[t]] + [lax.ppermute(stacked[t, : 2 * tok], "seq", pairs[d]) for d in range(1, devices)]
        mixed.append(attend_head(count, order, row, 1, tok))
    attn = jnp.concatenate(mixed, axis=1)
    weights = lax.all_gather(w_out, "seq", axis=1, tiled=True)
    terms = jnp.dot(attn, weights, preferred_element_type=jnp.float32)
    return lax.psum_scatter(terms.astype(jnp.bfloat16), "head", scatter_dimension=1, tiled=True)


def solution(mesh):
    devices, groups = mesh.shape["seq"], mesh.shape["head"]
    if devices & (devices - 1):
        raise ValueError("seq size")

    def body(queries, keys, values, frame_of_block, pair_mask, w_out):
        heads = queries.shape[1] // HD
        chosen = halves_body if (devices, groups) == (8, 4) and heads % (devices // 2) == 0 else gather_body
        return chosen(queries, keys, values, frame_of_block, pair_mask, w_out, devices)

    placed = (
        P("seq", "head"),
        P("seq", "head"),
        P("seq", "head"),
        P("seq"),
        P("seq", None),
        P("head", "seq"),
    )
    return jax.shard_map(body, mesh=mesh, in_specs=placed, out_specs=P("seq", "head"), check_vma=False)
```

```python
import functools
import math

import jax
import jax.numpy as jnp
from jax import lax
from jax.experimental import pallas as pl
from jax.experimental.pallas import tpu as pltpu
from jax.sharding import PartitionSpec as P


HD = 128
BLK = 256
SPAN = 4
META = 16
BOTH = ("seq", "head")


def attention_kernel(devices, asked, tok, count, order, *refs):
    pieces, out, q_all, k_all, v_all, peak, total, accum, sems = (refs[:devices], *refs[devices:])

    @pl.when(count[0] > 0)
    def _():
        copies = []
        for d in range(devices):
            parts = ((k_all, 0), (v_all, tok), (q_all, 2 * tok + META))
            for part, (held, first) in enumerate(parts[: 3 if d < asked else 2]):
                copies.append(
                    pltpu.make_async_copy(
                        pieces[d].at[pl.ds(first, tok)], held.at[pl.ds(d * tok, tok)], sems.at[3 * d + part]
                    )
                )
        for copy in copies:
            copy.start()
        for copy in copies:
            copy.wait()
        factor = math.log2(math.e) / math.sqrt(HD)
        key_blocks = devices * tok // BLK

        @pl.loop(0, asked * tok // BLK)
        def _(index):
            rows = pl.ds(pl.multiple_of(index * BLK, BLK), BLK)
            q = q_all[rows, :]
            seen = count[index]
            peak[...] = jnp.full_like(peak, -jnp.inf)
            total[...] = jnp.zeros_like(total)
            accum[...] = jnp.zeros_like(accum)

            def update(step, number):
                firsts = [
                    pl.multiple_of(order[index * key_blocks + step + u] * BLK, BLK) for u in range(number)
                ]
                scores = [
                    lax.dot_general(
                        q, k_all[pl.ds(first, BLK), :], (((1,), (1,)), ((), ())), preferred_element_type=jnp.float32
                    )
                    for first in firsts
                ]
                top = functools.reduce(jnp.maximum, [s[:, i : i + HD] for s in scores for i in (0, HD)])
                old = peak[...]
                new = jnp.maximum(old, jnp.broadcast_to(jnp.max(top, axis=1, keepdims=True), old.shape))
                peak[...] = new
                fade = jnp.exp2((old - new) * factor)
                sums, mixed = None, None
                for first, score in zip(firsts, scores):
                    left = jnp.exp2((score[:, :HD] - new) * factor)
                    right = jnp.exp2((score[:, HD:] - new) * factor)
                    weight = jnp.concatenate([left.astype(jnp.bfloat16), right.astype(jnp.bfloat16)], axis=1)
                    term = jnp.dot(weight, v_all[pl.ds(first, BLK), :], preferred_element_type=jnp.float32)
                    sums = left + right if sums is None else sums + (left + right)
                    mixed = term if mixed is None else mixed + term
                total[...] = total[...] * fade + sums
                accum[...] = accum[...] * fade + mixed

            @pl.loop(0, seen // 4)
            def _(step):
                update(step * 4, 4)

            @pl.when((seen & 2) != 0)
            def _():
                update((seen // 4) * 4, 2)

            @pl.when((seen & 1) != 0)
            def _():
                update(seen - 1, 1)

            @pl.when(seen > 0)
            def _():
                out[rows, :] = (accum[...] / jnp.sum(total[...], axis=1, keepdims=True)).astype(out.dtype)


def attend_head(count, order, pieces, asked, tok):
    devices = len(pieces)
    rows, keys = asked * tok, devices * tok
    return pl.pallas_call(
        functools.partial(attention_kernel, devices, asked, tok),
        out_shape=jax.ShapeDtypeStruct((rows, HD), jnp.bfloat16),
        in_specs=[pl.BlockSpec(memory_space=pltpu.SMEM)] * 2 + [pl.BlockSpec(memory_space=pl.ANY)] * devices,
        out_specs=pl.BlockSpec(memory_space=pltpu.VMEM),
        scratch_shapes=[
            pltpu.VMEM((rows, HD), jnp.bfloat16),
            pltpu.VMEM((keys, HD), jnp.bfloat16),
            pltpu.VMEM((keys, HD), jnp.bfloat16),
            pltpu.VMEM((BLK, HD), jnp.float32),
            pltpu.VMEM((BLK, HD), jnp.float32),
            pltpu.VMEM((BLK, HD), jnp.float32),
            pltpu.SemaphoreType.DMA((3 * devices,)),
        ],
        compiler_params=pltpu.CompilerParams(vmem_limit_bytes=24 << 20),
        cost_estimate=pl.CostEstimate(
            flops=4 * rows * keys * HD, bytes_accessed=2 * HD * (2 * rows + 2 * keys), transcendentals=rows * keys
        ),
        name="attend_head",
    )(count, order, *pieces)


def pack_kernel(group, share, tok, own, keys, values, queries, meta, *refs):
    number = group * share
    whole, short = refs[:number], refs[number : 2 * number - group]
    held, in_sems, out_sems = refs[2 * number - group :]
    rows = ((keys, 0, tok), (values, tok, tok), (meta, 2 * tok, META), (queries, 2 * tok + META, tok))
    takes, puts = [], []
    for c in range(group):
        for t in range(share):
            i = c * share + t
            first = pl.multiple_of(((own[0] ^ c) * share + t) * HD, HD)
            takes.append(
                [
                    pltpu.make_async_copy(
                        source if source is meta else source.at[:, pl.ds(first, HD)],
                        held.at[i, pl.ds(start, size)],
                        in_sems.at[4 * i + part],
                    )
                    for part, (source, start, size) in enumerate(rows)
                ]
            )
            puts.append([pltpu.make_async_copy(held.at[i], whole[i], out_sems.at[2 * i])])
            if t:
                part = held.at[i, pl.ds(0, 2 * tok + META)]
                puts[i].append(pltpu.make_async_copy(part, short[i - c - 1], out_sems.at[2 * i + 1]))
    for i in [c * share + t for t in range(share) for c in range(group)]:
        for copy in takes[i]:
            copy.start()
    for i in [c * share + t for t in range(share) for c in range(group)]:
        for copy in takes[i]:
            copy.wait()
        for copy in puts[i]:
            copy.start()
    for pair in puts:
        for copy in pair:
            copy.wait()


def pack(own, keys, values, queries, meta, group, share):
    tok = keys.shape[0]
    number = group * share
    sizes = [3 * tok + META] * number + [2 * tok + META] * (number - group)
    packed = pl.pallas_call(
        functools.partial(pack_kernel, group, share, tok),
        out_shape=[jax.ShapeDtypeStruct((size, HD), jnp.bfloat16) for size in sizes],
        in_specs=[pl.BlockSpec(memory_space=pltpu.SMEM)] + [pl.BlockSpec(memory_space=pltpu.HBM)] * 4,
        out_specs=[pl.BlockSpec(memory_space=pltpu.HBM)] * (2 * number - group),
        scratch_shapes=[
            pltpu.VMEM((number, 3 * tok + META, HD), jnp.bfloat16),
            pltpu.SemaphoreType.DMA((4 * number,)),
            pltpu.SemaphoreType.DMA((2 * number,)),
        ],
        compiler_params=pltpu.CompilerParams(vmem_limit_bytes=60 << 20),
        name="pack",
    )(own[None], keys, values, queries, meta)
    split = lambda flat, each: [flat[c * each : (c + 1) * each] for c in range(group)]
    return split(packed[:number], share), [[None, *row] for row in split(packed[number:], share - 1)]


def block_lists(k_frame, rows, held):
    number = held.shape[0]
    q_frame = k_frame[: rows.shape[0]]
    pick = (held[:, None] == jnp.arange(rows.shape[1], dtype=jnp.int32)[None, :]).astype(jnp.int32)
    link = jnp.sum(rows[:, None, :] * pick[None, :, :], axis=2)
    same = k_frame[None, :] == q_frame[:, None]
    seen = ((k_frame[None, :] <= q_frame[:, None]) & ((link == 1) | same)).astype(jnp.int32)
    spot = jnp.arange(number, dtype=jnp.int32)
    before = (spot[:, None] < spot[None, :]).astype(jnp.int32)
    rank = jnp.sum(seen[:, :, None] * before[None, :, :], axis=1)
    chosen = seen[:, :, None] * (rank[:, :, None] == spot[None, None, :]).astype(jnp.int32)
    order = jnp.sum(chosen * spot[None, :, None], axis=1)
    return jnp.sum(seen, axis=1), order.reshape(-1)


def halves_body(queries, keys, values, frame_of_block, pair_mask, w_out, devices):
    group = devices // 2
    tok, width = queries.shape
    heads = width // HD
    share = heads // group
    per_dev = frame_of_block.shape[0]
    near = -(-(SPAN - 1) // per_dev)
    seq, head = lax.axis_index("seq"), lax.axis_index("head")
    own = lax.rem(seq, group)
    half, side, core = seq // group, head // 2, lax.rem(head, 2)

    meta = jnp.concatenate([frame_of_block[:, None], pair_mask], axis=1).astype(jnp.bfloat16)
    blocks = pair_mask.shape[1]
    meta = jnp.pad(meta, ((0, META - per_dev), (0, HD - 1 - blocks)))
    whole, short = pack(own, keys, values, queries, meta, group, share)

    arrived = [[row[0]] + [None] * (devices - 1) for row in [[whole[0][t]] for t in range(share)]]
    for t in range(share):
        for d in range(1, devices):
            if d < group:
                piece, senders = whole[d][t], range(group if t == 0 else devices)
            elif t == 0:
                piece, senders = whole[d % group][t], range(group, devices)
            else:
                piece, senders = short[d % group][t], range(group + near)
            arrived[t][d] = lax.ppermute(piece, "seq", [(s, s ^ d) for s in senders])

    meta_rows = slice(2 * tok, 2 * tok + per_dev)
    told = [piece[meta_rows, : 1 + blocks] for piece in arrived[1]]
    for d in range(group, devices):
        told[d] = jnp.where(half == 0, arrived[0][d][meta_rows, : 1 + blocks], told[d])
    told = jnp.concatenate(told, axis=0).astype(jnp.int32)
    source = seq ^ jnp.arange(devices, dtype=jnp.int32)
    held = (source[:, None] * per_dev + jnp.arange(per_dev, dtype=jnp.int32)).reshape(-1)
    count, order = block_lists(told[:, 0], told[:, 1:], held)
    count_all = jnp.where(half == 0, count, 0)

    columns = w_out.shape[1]
    w_here = jnp.concatenate(
        [lax.dynamic_slice_in_dim(w_out, (own ^ e) * share * HD, share * HD, 0) for e in range(group)], axis=0
    )
    bounds = [columns * p // 6 for p in (0, 1, 3, 5, 6)]
    w_parts = [w_here[:, first:last] for first, last in zip(bounds, bounds[1:])]
    w_far = [lax.ppermute(part, "seq", [(s, s ^ group) for s in range(devices)]) for part in w_parts]

    mixed = [None] * share
    both = attend_head(count_all, order, arrived[0], devices, tok)
    for t in range(1, share):
        mixed[t] = attend_head(count, order, arrived[t], group, tok)
    back = lax.ppermute(both[group * tok :], "seq", [(s, s ^ group) for s in range(group)])
    mixed[0] = jnp.where(half == 0, both[: group * tok], back)

    gathered = [mixed, [], [], []]
    for t in range(share):
        for e in (1, 2):
            gathered[e].append(lax.ppermute(mixed[t], "seq", [(s, s ^ e) for s in range(devices)]))
        gathered[3].append(lax.ppermute(gathered[2][t], "seq", [(s, s ^ 1) for s in range(devices)]))
    attn = jnp.concatenate(
        [
            jnp.concatenate(
                [gathered[e][t][(d ^ e) * tok : ((d ^ e) + 1) * tok] for e in range(group) for t in range(share)],
                axis=1,
            )
            for d in range(group)
        ],
        axis=0,
    )

    pairs = [(s, h) for s in range(devices) for h in range(4)]

    def place(s, h):
        return s * 4 + h

    def finish(weights, near_side):
        sides = [(s, h) for s, h in pairs if (h // 2 == s // group) == near_side]
        terms = jnp.dot(attn, weights, preferred_element_type=jnp.float32)
        kept = lax.dynamic_slice_in_dim(terms, core * 2 * tok, 2 * tok, 0)
        given = lax.dynamic_slice_in_dim(terms, (1 - core) * 2 * tok, 2 * tok, 0).astype(jnp.bfloat16)
        got = lax.ppermute(given, "head", [(h, h ^ 1) for h in range(4)])
        kept = kept + got.astype(jnp.float32)
        moves = [(place(s, h ^ 2), place(s, h)) for s, h in sides]
        other = lax.ppermute(kept.astype(jnp.bfloat16), BOTH, moves)
        summed = (kept + other.astype(jnp.float32)).astype(jnp.bfloat16)
        ends = []
        for flip in range(2):
            moves = [
                (place(s, h), place(s ^ ((h % 2) * 2 + flip), (h // 2) * 2 + (s % group) // 2)) for s, h in sides
            ]
            ends.append(lax.ppermute(summed[flip * tok : (flip + 1) * tok], BOTH, moves))
        return ends

    near_ends = finish(w_here, True)
    far_sets = [jnp.concatenate(w_far[:2], axis=1), w_far[2], w_far[3]]
    far_parts = [finish(w, False) for w in far_sets]
    far_ends = [jnp.concatenate([part[flip] for part in far_parts], axis=1) for flip in range(2)]
    same, across = [jnp.where(half == side, n, f) for n, f in zip(near_ends, far_ends)]
    odd = lax.rem(seq, 2) == 1
    return jnp.concatenate([jnp.where(odd, across, same), jnp.where(odd, same, across)], axis=1)


def gather_body(queries, keys, values, frame_of_block, pair_mask, w_out, devices):
    tok, width = queries.shape
    heads = width // HD
    per_dev = frame_of_block.shape[0]
    seq = lax.axis_index("seq")
    meta = lax.all_gather(jnp.concatenate([frame_of_block[:, None], pair_mask], axis=1), "seq", axis=0, tiled=True)
    source = seq ^ jnp.arange(devices, dtype=jnp.int32)
    held = (source[:, None] * per_dev + jnp.arange(per_dev, dtype=jnp.int32)).reshape(-1)
    pick = (held[:, None] == jnp.arange(devices * per_dev, dtype=jnp.int32)[None, :]).astype(jnp.int32)
    k_frame = jnp.sum(pick * meta[None, :, 0], axis=1)
    count, order = block_lists(k_frame, pair_mask, held)
    split = [x.reshape(tok, heads, HD).transpose(1, 0, 2) for x in (keys, values, queries)]
    stacked = jnp.concatenate(split[:2] + [jnp.zeros((heads, META, HD), jnp.bfloat16), split[2]], axis=1)
    pairs = [[(s, s ^ d) for s in range(devices)] for d in range(devices)]
    mixed = []
    for t in range(heads):
        row = [stacked[t]] + [lax.ppermute(stacked[t, : 2 * tok], "seq", pairs[d]) for d in range(1, devices)]
        mixed.append(attend_head(count, order, row, 1, tok))
    attn = jnp.concatenate(mixed, axis=1)
    weights = lax.all_gather(w_out, "seq", axis=1, tiled=True)
    terms = jnp.dot(attn, weights, preferred_element_type=jnp.float32)
    return lax.psum_scatter(terms.astype(jnp.bfloat16), "head", scatter_dimension=1, tiled=True)


def solution(mesh):
    devices, groups = mesh.shape["seq"], mesh.shape["head"]
    if devices & (devices - 1):
        raise ValueError("seq size")
    placed = (
        P("seq", "head"),
        P("seq", "head"),
        P("seq", "head"),
        P("seq"),
        P("seq", None),
        P("head", "seq"),
    )

    def program(*arrays):
        heads = arrays[0].shape[1] // HD // groups
        halves = (devices, groups) == (8, 4) and heads % (devices // 2) == 0

        def body(*blocks):
            if not halves:
                return gather_body(*blocks, devices)
            return halves_body(*blocks, devices)

        step = jax.shard_map(body, mesh=mesh, in_specs=placed, out_specs=P("seq", "head"), check_vma=False)
        return step(*arrays)

    return program
```

```python
import functools
import math

import jax
import jax.numpy as jnp
from jax import lax
from jax.experimental import pallas as pl
from jax.experimental.pallas import tpu as pltpu
from jax.sharding import PartitionSpec as P


HD = 128
BLK = 256
SPAN = 4
META = 16
BOTH = ("seq", "head")


def attention_kernel(devices, asked, tok, count, order, *refs):
    pieces, out, q_all, k_all, v_all, peak, total, accum, sems = (refs[:devices], *refs[devices:])

    @pl.when(count[0] > 0)
    def _():
        copies = []
        for d in range(devices):
            parts = ((k_all, 0), (v_all, tok), (q_all, 2 * tok + META))
            for part, (held, first) in enumerate(parts[: 3 if d < asked else 2]):
                copies.append(
                    pltpu.make_async_copy(
                        pieces[d].at[pl.ds(first, tok)], held.at[pl.ds(d * tok, tok)], sems.at[3 * d + part]
                    )
                )
        for copy in copies:
            copy.start()
        for copy in copies:
            copy.wait()
        factor = math.log2(math.e) / math.sqrt(HD)
        key_blocks = devices * tok // BLK

        @pl.loop(0, asked * tok // BLK)
        def _(index):
            rows = pl.ds(pl.multiple_of(index * BLK, BLK), BLK)
            q = q_all[rows, :]
            seen = count[index]
            peak[...] = jnp.full_like(peak, -jnp.inf)
            total[...] = jnp.zeros_like(total)
            accum[...] = jnp.zeros_like(accum)

            def update(step, number):
                firsts = [
                    pl.multiple_of(order[index * key_blocks + step + u] * BLK, BLK) for u in range(number)
                ]
                scores = [
                    lax.dot_general(
                        q, k_all[pl.ds(first, BLK), :], (((1,), (1,)), ((), ())), preferred_element_type=jnp.float32
                    )
                    for first in firsts
                ]
                top = functools.reduce(jnp.maximum, [s[:, i : i + HD] for s in scores for i in (0, HD)])
                old = peak[...]
                new = jnp.maximum(old, jnp.broadcast_to(jnp.max(top, axis=1, keepdims=True), old.shape))
                peak[...] = new
                fade = jnp.exp2((old - new) * factor)
                sums, mixed = None, None
                for first, score in zip(firsts, scores):
                    left = jnp.exp2((score[:, :HD] - new) * factor)
                    right = jnp.exp2((score[:, HD:] - new) * factor)
                    weight = jnp.concatenate([left.astype(jnp.bfloat16), right.astype(jnp.bfloat16)], axis=1)
                    term = jnp.dot(weight, v_all[pl.ds(first, BLK), :], preferred_element_type=jnp.float32)
                    sums = left + right if sums is None else sums + (left + right)
                    mixed = term if mixed is None else mixed + term
                total[...] = total[...] * fade + sums
                accum[...] = accum[...] * fade + mixed

            @pl.loop(0, seen // 4)
            def _(step):
                update(step * 4, 4)

            @pl.when((seen & 2) != 0)
            def _():
                update((seen // 4) * 4, 2)

            @pl.when((seen & 1) != 0)
            def _():
                update(seen - 1, 1)

            @pl.when(seen > 0)
            def _():
                out[rows, :] = (accum[...] / jnp.sum(total[...], axis=1, keepdims=True)).astype(out.dtype)


def attend_head(count, order, pieces, asked, tok):
    devices = len(pieces)
    rows, keys = asked * tok, devices * tok
    return pl.pallas_call(
        functools.partial(attention_kernel, devices, asked, tok),
        out_shape=jax.ShapeDtypeStruct((rows, HD), jnp.bfloat16),
        in_specs=[pl.BlockSpec(memory_space=pltpu.SMEM)] * 2 + [pl.BlockSpec(memory_space=pl.ANY)] * devices,
        out_specs=pl.BlockSpec(memory_space=pltpu.VMEM),
        scratch_shapes=[
            pltpu.VMEM((rows, HD), jnp.bfloat16),
            pltpu.VMEM((keys, HD), jnp.bfloat16),
            pltpu.VMEM((keys, HD), jnp.bfloat16),
            pltpu.VMEM((BLK, HD), jnp.float32),
            pltpu.VMEM((BLK, HD), jnp.float32),
            pltpu.VMEM((BLK, HD), jnp.float32),
            pltpu.SemaphoreType.DMA((3 * devices,)),
        ],
        compiler_params=pltpu.CompilerParams(vmem_limit_bytes=24 << 20),
        cost_estimate=pl.CostEstimate(
            flops=4 * rows * keys * HD, bytes_accessed=2 * HD * (2 * rows + 2 * keys), transcendentals=rows * keys
        ),
        name="attend_head",
    )(count, order, *pieces)


def pack_kernel(group, share, tok, own, keys, values, queries, meta, *refs):
    number = group * share
    whole, short = refs[:number], refs[number : 2 * number - group]
    held, in_sems, out_sems = refs[2 * number - group :]
    rows = ((keys, 0, tok), (values, tok, tok), (meta, 2 * tok, META), (queries, 2 * tok + META, tok))
    takes, puts = [], []
    for c in range(group):
        for t in range(share):
            i = c * share + t
            first = pl.multiple_of(((own[0] ^ c) * share + t) * HD, HD)
            takes.append(
                [
                    pltpu.make_async_copy(
                        source if source is meta else source.at[:, pl.ds(first, HD)],
                        held.at[i, pl.ds(start, size)],
                        in_sems.at[4 * i + part],
                    )
                    for part, (source, start, size) in enumerate(rows)
                ]
            )
            puts.append([pltpu.make_async_copy(held.at[i], whole[i], out_sems.at[2 * i])])
            if t:
                part = held.at[i, pl.ds(0, 2 * tok + META)]
                puts[i].append(pltpu.make_async_copy(part, short[i - c - 1], out_sems.at[2 * i + 1]))
    for i in [c * share + t for t in range(share) for c in range(group)]:
        for copy in takes[i]:
            copy.start()
    for i in [c * share + t for t in range(share) for c in range(group)]:
        for copy in takes[i]:
            copy.wait()
        for copy in puts[i]:
            copy.start()
    for pair in puts:
        for copy in pair:
            copy.wait()


def pack(own, keys, values, queries, meta, group, share):
    tok = keys.shape[0]
    number = group * share
    sizes = [3 * tok + META] * number + [2 * tok + META] * (number - group)
    packed = pl.pallas_call(
        functools.partial(pack_kernel, group, share, tok),
        out_shape=[jax.ShapeDtypeStruct((size, HD), jnp.bfloat16) for size in sizes],
        in_specs=[pl.BlockSpec(memory_space=pltpu.SMEM)] + [pl.BlockSpec(memory_space=pltpu.HBM)] * 4,
        out_specs=[pl.BlockSpec(memory_space=pltpu.HBM)] * (2 * number - group),
        scratch_shapes=[
            pltpu.VMEM((number, 3 * tok + META, HD), jnp.bfloat16),
            pltpu.SemaphoreType.DMA((4 * number,)),
            pltpu.SemaphoreType.DMA((2 * number,)),
        ],
        compiler_params=pltpu.CompilerParams(vmem_limit_bytes=60 << 20),
        name="pack",
    )(own[None], keys, values, queries, meta)
    split = lambda flat, each: [flat[c * each : (c + 1) * each] for c in range(group)]
    return split(packed[:number], share), [[None, *row] for row in split(packed[number:], share - 1)]


def block_lists(k_frame, rows, held):
    number = held.shape[0]
    q_frame = k_frame[: rows.shape[0]]
    pick = (held[:, None] == jnp.arange(rows.shape[1], dtype=jnp.int32)[None, :]).astype(jnp.int32)
    link = jnp.sum(rows[:, None, :] * pick[None, :, :], axis=2)
    same = k_frame[None, :] == q_frame[:, None]
    seen = ((k_frame[None, :] <= q_frame[:, None]) & ((link == 1) | same)).astype(jnp.int32)
    spot = jnp.arange(number, dtype=jnp.int32)
    before = (spot[:, None] < spot[None, :]).astype(jnp.int32)
    rank = jnp.sum(seen[:, :, None] * before[None, :, :], axis=1)
    chosen = seen[:, :, None] * (rank[:, :, None] == spot[None, None, :]).astype(jnp.int32)
    order = jnp.sum(chosen * spot[None, :, None], axis=1)
    return jnp.sum(seen, axis=1), order.reshape(-1)


def halves_body(queries, keys, values, frame_of_block, pair_mask, w_out, devices):
    group = devices // 2
    tok, width = queries.shape
    heads = width // HD
    share = heads // group
    per_dev = frame_of_block.shape[0]
    near = -(-(SPAN - 1) // per_dev)
    seq, head = lax.axis_index("seq"), lax.axis_index("head")
    own = lax.rem(seq, group)
    half, side, core = seq // group, head // 2, lax.rem(head, 2)

    meta = jnp.concatenate([frame_of_block[:, None], pair_mask], axis=1).astype(jnp.bfloat16)
    blocks = pair_mask.shape[1]
    meta = jnp.pad(meta, ((0, META - per_dev), (0, HD - 1 - blocks)))
    whole, short = pack(own, keys, values, queries, meta, group, share)

    arrived = [[row[0]] + [None] * (devices - 1) for row in [[whole[0][t]] for t in range(share)]]
    for t in range(share):
        for d in range(1, devices):
            if d < group:
                piece, senders = whole[d][t], range(group if t == 0 else devices)
            elif t == 0:
                piece, senders = whole[d % group][t], range(group, devices)
            else:
                piece, senders = short[d % group][t], range(group + near)
            arrived[t][d] = lax.ppermute(piece, "seq", [(s, s ^ d) for s in senders])

    meta_rows = slice(2 * tok, 2 * tok + per_dev)
    told = [piece[meta_rows, : 1 + blocks] for piece in arrived[1]]
    for d in range(group, devices):
        told[d] = jnp.where(half == 0, arrived[0][d][meta_rows, : 1 + blocks], told[d])
    told = jnp.concatenate(told, axis=0).astype(jnp.int32)
    source = seq ^ jnp.arange(devices, dtype=jnp.int32)
    held = (source[:, None] * per_dev + jnp.arange(per_dev, dtype=jnp.int32)).reshape(-1)
    count, order = block_lists(told[:, 0], told[:, 1:], held)
    count_all = jnp.where(half == 0, count, 0)

    columns = w_out.shape[1]
    w_here = jnp.concatenate(
        [lax.dynamic_slice_in_dim(w_out, (own ^ e) * share * HD, share * HD, 0) for e in range(group)], axis=0
    )
    bounds = [columns * p // 6 for p in (0, 1, 3, 5, 6)]
    w_parts = [w_here[:, first:last] for first, last in zip(bounds, bounds[1:])]
    w_far = [lax.ppermute(part, "seq", [(s, s ^ group) for s in range(devices)]) for part in w_parts]

    mixed = [None] * share
    both = attend_head(count_all, order, arrived[0], devices, tok)
    for t in range(1, share):
        mixed[t] = attend_head(count, order, arrived[t], group, tok)
    back = lax.ppermute(both[group * tok :], "seq", [(s, s ^ group) for s in range(group)])
    mixed[0] = jnp.where(half == 0, both[: group * tok], back)

    gathered = [mixed, [], [], []]
    for t in range(share):
        for e in (1, 2):
            gathered[e].append(lax.ppermute(mixed[t], "seq", [(s, s ^ e) for s in range(devices)]))
        gathered[3].append(lax.ppermute(gathered[2][t], "seq", [(s, s ^ 1) for s in range(devices)]))
    attn = jnp.concatenate(
        [
            jnp.concatenate(
                [gathered[e][t][(d ^ e) * tok : ((d ^ e) + 1) * tok] for e in range(group) for t in range(share)],
                axis=1,
            )
            for d in range(group)
        ],
        axis=0,
    )

    def place(s, h):
        return s * 4 + h

    def moves(flip, turn):
        return [
            (place(s, h), place(s ^ ((h % 2) * 2 + flip), ((h // 2) ^ turn) * 2 + (s % group) // 2))
            for s in range(devices)
            for h in range(4)
        ]

    ends = [[], []]
    for p in range(2):
        first, last = bounds[2 * p], bounds[2 * p + 2]
        weights = jnp.concatenate([w_here[:, first:last], *w_far[2 * p : 2 * p + 2]], axis=1)
        if p:
            weights = lax.optimization_barrier((weights, parts))[0]
        terms = jnp.dot(attn, weights, preferred_element_type=jnp.float32)
        kept = lax.dynamic_slice_in_dim(terms, core * 2 * tok, 2 * tok, 0)
        given = lax.dynamic_slice_in_dim(terms, (1 - core) * 2 * tok, 2 * tok, 0).astype(jnp.bfloat16)
        got = lax.ppermute(given, "head", [(h, h ^ 1) for h in range(4)])
        summed = (kept + got.astype(jnp.float32)).astype(jnp.bfloat16)
        here, far = summed[:, : last - first], summed[:, last - first :]
        parts = (jnp.where(half == side, here, far), jnp.where(half == side, far, here))
        for flip in range(2):
            rows = slice(flip * tok, (flip + 1) * tok)
            got = [lax.ppermute(parts[turn][rows], BOTH, moves(flip, turn)) for turn in (1, 0)]
            ends[flip].append((got[0].astype(jnp.float32) + got[1].astype(jnp.float32)).astype(jnp.bfloat16))
    same, across = [jnp.concatenate(pieces, axis=1) for pieces in ends]
    odd = lax.rem(seq, 2) == 1
    return jnp.concatenate([jnp.where(odd, across, same), jnp.where(odd, same, across)], axis=1)


def gather_body(queries, keys, values, frame_of_block, pair_mask, w_out, devices):
    tok, width = queries.shape
    heads = width // HD
    per_dev = frame_of_block.shape[0]
    seq = lax.axis_index("seq")
    meta = lax.all_gather(jnp.concatenate([frame_of_block[:, None], pair_mask], axis=1), "seq", axis=0, tiled=True)
    source = seq ^ jnp.arange(devices, dtype=jnp.int32)
    held = (source[:, None] * per_dev + jnp.arange(per_dev, dtype=jnp.int32)).reshape(-1)
    pick = (held[:, None] == jnp.arange(devices * per_dev, dtype=jnp.int32)[None, :]).astype(jnp.int32)
    k_frame = jnp.sum(pick * meta[None, :, 0], axis=1)
    count, order = block_lists(k_frame, pair_mask, held)
    split = [x.reshape(tok, heads, HD).transpose(1, 0, 2) for x in (keys, values, queries)]
    stacked = jnp.concatenate(split[:2] + [jnp.zeros((heads, META, HD), jnp.bfloat16), split[2]], axis=1)
    pairs = [[(s, s ^ d) for s in range(devices)] for d in range(devices)]
    mixed = []
    for t in range(heads):
        row = [stacked[t]] + [lax.ppermute(stacked[t, : 2 * tok], "seq", pairs[d]) for d in range(1, devices)]
        mixed.append(attend_head(count, order, row, 1, tok))
    attn = jnp.concatenate(mixed, axis=1)
    weights = lax.all_gather(w_out, "seq", axis=1, tiled=True)
    terms = jnp.dot(attn, weights, preferred_element_type=jnp.float32)
    return lax.psum_scatter(terms.astype(jnp.bfloat16), "head", scatter_dimension=1, tiled=True)


def solution(mesh):
    devices, groups = mesh.shape["seq"], mesh.shape["head"]
    if devices & (devices - 1):
        raise ValueError("seq size")
    placed = (
        P("seq", "head"),
        P("seq", "head"),
        P("seq", "head"),
        P("seq"),
        P("seq", None),
        P("head", "seq"),
    )

    def program(*arrays):
        heads = arrays[0].shape[1] // HD // groups
        halves = (devices, groups) == (8, 4) and heads % (devices // 2) == 0

        def body(*blocks):
            if not halves:
                return gather_body(*blocks, devices)
            return halves_body(*blocks, devices)

        step = jax.shard_map(body, mesh=mesh, in_specs=placed, out_specs=P("seq", "head"), check_vma=False)
        return step(*arrays)

    return program
```

```python
import functools
import math

import jax
import jax.numpy as jnp
from jax import lax
from jax.experimental import pallas as pl
from jax.experimental.pallas import tpu as pltpu
from jax.sharding import PartitionSpec as P


HD = 128
BLK = 256
SPAN = 4
META = 16
BOTH = ("seq", "head")


def attention_kernel(devices, asked, tok, count, order, *refs):
    pieces, out, q_all, k_all, v_all, peak, total, accum, sems = (refs[:devices], *refs[devices:])

    @pl.when(count[0] > 0)
    def _():
        copies = []
        for d in range(devices):
            parts = ((k_all, 0), (v_all, tok), (q_all, 2 * tok + META))
            for part, (held, first) in enumerate(parts[: 3 if d < asked else 2]):
                copies.append(
                    pltpu.make_async_copy(
                        pieces[d].at[pl.ds(first, tok)], held.at[pl.ds(d * tok, tok)], sems.at[3 * d + part]
                    )
                )
        for copy in copies:
            copy.start()
        for copy in copies:
            copy.wait()
        factor = math.log2(math.e) / math.sqrt(HD)
        key_blocks = devices * tok // BLK

        @pl.loop(0, asked * tok // BLK)
        def _(index):
            rows = pl.ds(pl.multiple_of(index * BLK, BLK), BLK)
            q = q_all[rows, :]
            seen = count[index]
            peak[...] = jnp.full_like(peak, -jnp.inf)
            total[...] = jnp.zeros_like(total)
            accum[...] = jnp.zeros_like(accum)

            def update(step, number):
                firsts = [
                    pl.multiple_of(order[index * key_blocks + step + u] * BLK, BLK) for u in range(number)
                ]
                scores = [
                    lax.dot_general(
                        q, k_all[pl.ds(first, BLK), :], (((1,), (1,)), ((), ())), preferred_element_type=jnp.float32
                    )
                    for first in firsts
                ]
                top = functools.reduce(jnp.maximum, [s[:, i : i + HD] for s in scores for i in (0, HD)])
                old = peak[...]
                new = jnp.maximum(old, jnp.broadcast_to(jnp.max(top, axis=1, keepdims=True), old.shape))
                peak[...] = new
                fade = jnp.exp2((old - new) * factor)
                sums, mixed = None, None
                for first, score in zip(firsts, scores):
                    left = jnp.exp2((score[:, :HD] - new) * factor)
                    right = jnp.exp2((score[:, HD:] - new) * factor)
                    weight = jnp.concatenate([left.astype(jnp.bfloat16), right.astype(jnp.bfloat16)], axis=1)
                    term = jnp.dot(weight, v_all[pl.ds(first, BLK), :], preferred_element_type=jnp.float32)
                    sums = left + right if sums is None else sums + (left + right)
                    mixed = term if mixed is None else mixed + term
                total[...] = total[...] * fade + sums
                accum[...] = accum[...] * fade + mixed

            @pl.loop(0, seen // 4)
            def _(step):
                update(step * 4, 4)

            @pl.when((seen & 2) != 0)
            def _():
                update((seen // 4) * 4, 2)

            @pl.when((seen & 1) != 0)
            def _():
                update(seen - 1, 1)

            @pl.when(seen > 0)
            def _():
                out[rows, :] = (accum[...] / jnp.sum(total[...], axis=1, keepdims=True)).astype(out.dtype)


def attend_head(count, order, pieces, asked, tok):
    devices = len(pieces)
    rows, keys = asked * tok, devices * tok
    return pl.pallas_call(
        functools.partial(attention_kernel, devices, asked, tok),
        out_shape=jax.ShapeDtypeStruct((rows, HD), jnp.bfloat16),
        in_specs=[pl.BlockSpec(memory_space=pltpu.SMEM)] * 2 + [pl.BlockSpec(memory_space=pl.ANY)] * devices,
        out_specs=pl.BlockSpec(memory_space=pltpu.VMEM),
        scratch_shapes=[
            pltpu.VMEM((rows, HD), jnp.bfloat16),
            pltpu.VMEM((keys, HD), jnp.bfloat16),
            pltpu.VMEM((keys, HD), jnp.bfloat16),
            pltpu.VMEM((BLK, HD), jnp.float32),
            pltpu.VMEM((BLK, HD), jnp.float32),
            pltpu.VMEM((BLK, HD), jnp.float32),
            pltpu.SemaphoreType.DMA((3 * devices,)),
        ],
        compiler_params=pltpu.CompilerParams(vmem_limit_bytes=24 << 20),
        cost_estimate=pl.CostEstimate(
            flops=4 * rows * keys * HD, bytes_accessed=2 * HD * (2 * rows + 2 * keys), transcendentals=rows * keys
        ),
        name="attend_head",
    )(count, order, *pieces)


def pack_kernel(group, share, tok, own, keys, values, queries, meta, *refs):
    number = group * share
    whole, short = refs[:number], refs[number : 2 * number - group]
    held, in_sems, out_sems = refs[2 * number - group :]
    rows = ((keys, 0, tok), (values, tok, tok), (meta, 2 * tok, META), (queries, 2 * tok + META, tok))
    takes, puts = [], []
    for c in range(group):
        for t in range(share):
            i = c * share + t
            first = pl.multiple_of(((own[0] ^ c) * share + t) * HD, HD)
            takes.append(
                [
                    pltpu.make_async_copy(
                        source if source is meta else source.at[:, pl.ds(first, HD)],
                        held.at[i, pl.ds(start, size)],
                        in_sems.at[4 * i + part],
                    )
                    for part, (source, start, size) in enumerate(rows)
                ]
            )
            puts.append([pltpu.make_async_copy(held.at[i], whole[i], out_sems.at[2 * i])])
            if t:
                part = held.at[i, pl.ds(0, 2 * tok + META)]
                puts[i].append(pltpu.make_async_copy(part, short[i - c - 1], out_sems.at[2 * i + 1]))
    for i in [c * share + t for t in range(share) for c in range(group)]:
        for copy in takes[i]:
            copy.start()
    for i in [c * share + t for t in range(share) for c in range(group)]:
        for copy in takes[i]:
            copy.wait()
        for copy in puts[i]:
            copy.start()
    for pair in puts:
        for copy in pair:
            copy.wait()


def pack(own, keys, values, queries, meta, group, share):
    tok = keys.shape[0]
    number = group * share
    sizes = [3 * tok + META] * number + [2 * tok + META] * (number - group)
    packed = pl.pallas_call(
        functools.partial(pack_kernel, group, share, tok),
        out_shape=[jax.ShapeDtypeStruct((size, HD), jnp.bfloat16) for size in sizes],
        in_specs=[pl.BlockSpec(memory_space=pltpu.SMEM)] + [pl.BlockSpec(memory_space=pltpu.HBM)] * 4,
        out_specs=[pl.BlockSpec(memory_space=pltpu.HBM)] * (2 * number - group),
        scratch_shapes=[
            pltpu.VMEM((number, 3 * tok + META, HD), jnp.bfloat16),
            pltpu.SemaphoreType.DMA((4 * number,)),
            pltpu.SemaphoreType.DMA((2 * number,)),
        ],
        compiler_params=pltpu.CompilerParams(vmem_limit_bytes=60 << 20),
        name="pack",
    )(own[None], keys, values, queries, meta)
    split = lambda flat, each: [flat[c * each : (c + 1) * each] for c in range(group)]
    return split(packed[:number], share), [[None, *row] for row in split(packed[number:], share - 1)]


def block_lists(k_frame, rows, held):
    number = held.shape[0]
    q_frame = k_frame[: rows.shape[0]]
    pick = (held[:, None] == jnp.arange(rows.shape[1], dtype=jnp.int32)[None, :]).astype(jnp.int32)
    link = jnp.sum(rows[:, None, :] * pick[None, :, :], axis=2)
    same = k_frame[None, :] == q_frame[:, None]
    seen = ((k_frame[None, :] <= q_frame[:, None]) & ((link == 1) | same)).astype(jnp.int32)
    spot = jnp.arange(number, dtype=jnp.int32)
    before = (spot[:, None] < spot[None, :]).astype(jnp.int32)
    rank = jnp.sum(seen[:, :, None] * before[None, :, :], axis=1)
    chosen = seen[:, :, None] * (rank[:, :, None] == spot[None, None, :]).astype(jnp.int32)
    order = jnp.sum(chosen * spot[None, :, None], axis=1)
    return jnp.sum(seen, axis=1), order.reshape(-1)


def halves_body(queries, keys, values, frame_of_block, pair_mask, w_out, devices):
    group = devices // 2
    tok, width = queries.shape
    heads = width // HD
    share = heads // group
    per_dev = frame_of_block.shape[0]
    near = -(-(SPAN - 1) // per_dev)
    seq, head = lax.axis_index("seq"), lax.axis_index("head")
    own = lax.rem(seq, group)
    half, side, core = seq // group, head // 2, lax.rem(head, 2)

    meta = jnp.concatenate([frame_of_block[:, None], pair_mask], axis=1).astype(jnp.bfloat16)
    blocks = pair_mask.shape[1]
    meta = jnp.pad(meta, ((0, META - per_dev), (0, HD - 1 - blocks)))
    whole, short = pack(own, keys, values, queries, meta, group, share)

    arrived = [[row[0]] + [None] * (devices - 1) for row in [[whole[0][t]] for t in range(share)]]
    for t in range(share):
        for d in range(1, devices):
            if d < group:
                piece, senders = whole[d][t], range(group if t == 0 else devices)
            elif t == 0:
                piece, senders = whole[d % group][t], range(group, devices)
            else:
                piece, senders = short[d % group][t], range(group + near)
            arrived[t][d] = lax.ppermute(piece, "seq", [(s, s ^ d) for s in senders])

    meta_rows = slice(2 * tok, 2 * tok + per_dev)
    told = [piece[meta_rows, : 1 + blocks] for piece in arrived[1]]
    for d in range(group, devices):
        told[d] = jnp.where(half == 0, arrived[0][d][meta_rows, : 1 + blocks], told[d])
    told = jnp.concatenate(told, axis=0).astype(jnp.int32)
    source = seq ^ jnp.arange(devices, dtype=jnp.int32)
    held = (source[:, None] * per_dev + jnp.arange(per_dev, dtype=jnp.int32)).reshape(-1)
    count, order = block_lists(told[:, 0], told[:, 1:], held)
    count_all = jnp.where(half == 0, count, 0)

    columns = w_out.shape[1]
    w_here = jnp.concatenate(
        [lax.dynamic_slice_in_dim(w_out, (own ^ e) * share * HD, share * HD, 0) for e in range(group)], axis=0
    )
    bounds = [columns * p // 6 for p in (0, 1, 3, 5, 6)]
    w_parts = [w_here[:, first:last] for first, last in zip(bounds, bounds[1:])]
    w_far = [lax.ppermute(part, "seq", [(s, s ^ group) for s in range(devices)]) for part in w_parts]

    mixed = [None] * share
    both = attend_head(count_all, order, arrived[0], devices, tok)
    for t in range(1, share):
        mixed[t] = attend_head(count, order, arrived[t], group, tok)
    back = lax.ppermute(both[group * tok :], "seq", [(s, s ^ group) for s in range(group)])
    mixed[0] = jnp.where(half == 0, both[: group * tok], back)

    gathered = [mixed, [], [], []]
    for t in range(share):
        for e in (1, 2):
            gathered[e].append(lax.ppermute(mixed[t], "seq", [(s, s ^ e) for s in range(devices)]))
        gathered[3].append(lax.ppermute(gathered[2][t], "seq", [(s, s ^ 1) for s in range(devices)]))
    attn = jnp.concatenate(
        [
            jnp.concatenate(
                [gathered[e][t][(d ^ e) * tok : ((d ^ e) + 1) * tok] for e in range(group) for t in range(share)],
                axis=1,
            )
            for d in range(group)
        ],
        axis=0,
    )

    def place(s, h):
        return s * 4 + h

    def moves(flip, turn):
        return [
            (place(s, h), place(s ^ ((h % 2) * 2 + flip), ((h // 2) ^ turn) * 2 + (s % group) // 2))
            for s in range(devices)
            for h in range(4)
        ]

    ends = [[], []]
    for p in range(2):
        first, last = bounds[2 * p], bounds[2 * p + 2]
        arrived_w = w_far[2 * p : 2 * p + 2]
        if p:
            arrived_w = lax.optimization_barrier((*arrived_w, *ends[0]))[:2]
        weights = jnp.concatenate([w_here[:, first:last], *arrived_w], axis=1)
        terms = jnp.dot(attn, weights, preferred_element_type=jnp.float32)
        kept = lax.dynamic_slice_in_dim(terms, core * 2 * tok, 2 * tok, 0)
        given = lax.dynamic_slice_in_dim(terms, (1 - core) * 2 * tok, 2 * tok, 0).astype(jnp.bfloat16)
        got = lax.ppermute(given, "head", [(h, h ^ 1) for h in range(4)])
        summed = (kept + got.astype(jnp.float32)).astype(jnp.bfloat16)
        here, far = summed[:, : last - first], summed[:, last - first :]
        parts = (jnp.where(half == side, here, far), jnp.where(half == side, far, here))
        for flip in range(2):
            rows = slice(flip * tok, (flip + 1) * tok)
            got = [lax.ppermute(parts[turn][rows], BOTH, moves(flip, turn)) for turn in (1, 0)]
            ends[flip].append((got[0].astype(jnp.float32) + got[1].astype(jnp.float32)).astype(jnp.bfloat16))
    same, across = [jnp.concatenate(pieces, axis=1) for pieces in ends]
    odd = lax.rem(seq, 2) == 1
    return jnp.concatenate([jnp.where(odd, across, same), jnp.where(odd, same, across)], axis=1)


def gather_body(queries, keys, values, frame_of_block, pair_mask, w_out, devices):
    tok, width = queries.shape
    heads = width // HD
    per_dev = frame_of_block.shape[0]
    seq = lax.axis_index("seq")
    meta = lax.all_gather(jnp.concatenate([frame_of_block[:, None], pair_mask], axis=1), "seq", axis=0, tiled=True)
    source = seq ^ jnp.arange(devices, dtype=jnp.int32)
    held = (source[:, None] * per_dev + jnp.arange(per_dev, dtype=jnp.int32)).reshape(-1)
    pick = (held[:, None] == jnp.arange(devices * per_dev, dtype=jnp.int32)[None, :]).astype(jnp.int32)
    k_frame = jnp.sum(pick * meta[None, :, 0], axis=1)
    count, order = block_lists(k_frame, pair_mask, held)
    split = [x.reshape(tok, heads, HD).transpose(1, 0, 2) for x in (keys, values, queries)]
    stacked = jnp.concatenate(split[:2] + [jnp.zeros((heads, META, HD), jnp.bfloat16), split[2]], axis=1)
    pairs = [[(s, s ^ d) for s in range(devices)] for d in range(devices)]
    mixed = []
    for t in range(heads):
        row = [stacked[t]] + [lax.ppermute(stacked[t, : 2 * tok], "seq", pairs[d]) for d in range(1, devices)]
        mixed.append(attend_head(count, order, row, 1, tok))
    attn = jnp.concatenate(mixed, axis=1)
    weights = lax.all_gather(w_out, "seq", axis=1, tiled=True)
    terms = jnp.dot(attn, weights, preferred_element_type=jnp.float32)
    return lax.psum_scatter(terms.astype(jnp.bfloat16), "head", scatter_dimension=1, tiled=True)


def solution(mesh):
    devices, groups = mesh.shape["seq"], mesh.shape["head"]
    if devices & (devices - 1):
        raise ValueError("seq size")
    placed = (
        P("seq", "head"),
        P("seq", "head"),
        P("seq", "head"),
        P("seq"),
        P("seq", None),
        P("head", "seq"),
    )

    def program(*arrays):
        heads = arrays[0].shape[1] // HD // groups
        halves = (devices, groups) == (8, 4) and heads % (devices // 2) == 0

        def body(*blocks):
            if not halves:
                return gather_body(*blocks, devices)
            return halves_body(*blocks, devices)

        step = jax.shard_map(body, mesh=mesh, in_specs=placed, out_specs=P("seq", "head"), check_vma=False)
        return step(*arrays)

    return program
```
